128 devices in a mesh: seq: 16 (over z, y_hi, core), fsdp: 8 (over y_lo, x).
Axes of the slice: x: 4, y: 4 (y_hi: 2, y_lo: 2; y = y_hi * 2 + y_lo), z: 4, core: 2. Of those that a mesh axis runs over, the one named last changes fastest.
Arguments:
- patches: bfloat16 [8, 2048, 3072], P('fsdp', 'seq'), may hold values from -6 to 6
- weight_codes: int32 [3072, 3072], P('fsdp'), may hold values from -448 to 448
- block_scales: float32 [24, 24], P('fsdp'), may hold values from 2.5e-05 to 0.0001
- key_proj: bfloat16 [8, 2048, 3072], P('fsdp', 'seq'), may hold values from -6 to 6
- value_proj: bfloat16 [8, 2048, 3072], P('fsdp', 'seq'), may hold values from -6 to 6
- query_gain: float32 [3072], replicated, may hold values from 1 to 10
- key_gain: float32 [3072], replicated, may hold values from 1 to 10
Outputs:
- attended: bfloat16 [8, 2048, 3072], P('fsdp', 'seq')
The draws below stay inside these ranges and needn't reach their ends.
All inputs are finite; a program needn't handle non-finite values.
Results may differ from the reference program's by a relative error of at most 0.007.
The reference program's roundings to bfloat16 on the way count: a program that leaves them out, or rounds other values in their place, can miss the bound.
Values may be sent and summed in bfloat16 or wider, within the bound.
A program may use at most 192 MiB of HBM per device.

```python
import math
import jax
import jax.numpy as jnp
from jax import lax

D = 3072
HEADS = 48
HDIM = 64
BLOCK = 128
IMAGES = 8
SEQ = 2048


def gain_values(key, which):
    own_key = jax.random.fold_in(key, which)
    values = jnp.exp(jax.random.uniform(own_key, (HEADS, HDIM), minval=0.0, maxval=math.log(3.0)))
    return values.reshape(HEADS * HDIM).astype(jnp.float32)


def draw_query_gain(key, part):
    return gain_values(key, 1)


def draw_key_gain(key, part):
    return gain_values(key, 2)


def touch_ends(drawn, rng, least, high):
    index_at = [jax.random.randint(jax.random.fold_in(rng, axis), (), 0, length) for axis, length in enumerate(drawn.shape)]
    longest = drawn.shape.index(max(drawn.shape))
    next_to = index_at[:longest] + [(index_at[longest] + 1) % drawn.shape[longest]] + index_at[longest + 1:]
    return drawn.at[tuple(index_at)].set(least).at[tuple(next_to)].set(high)


def block_scale(key, dims, pieces, smallest, high):
    gain, own = 1.0, jax.random.fold_in(key, 6)
    for dim, shards_of in pieces:
        steps = jnp.exp(jax.random.uniform(jax.random.fold_in(own, dim), (shards_of,), jnp.float32, smallest / len(pieces), high / len(pieces)))
        gain = gain * jnp.repeat(steps, dims[dim] // shards_of).reshape([-1 if axis == dim else 1 for axis in range(len(dims))])
    return gain


def bell_draw(key, shape, deviation, limit, shards=(), held_as=jnp.bfloat16):
    values = deviation * jax.random.normal(key, shape, jnp.float32)
    if shards:
        values = values * block_scale(key, shape, shards, -0.22, 0.18)
    return jnp.clip(values, -limit, limit).astype(held_as)


def setup_inputs(seed: int = 0) -> dict:
    keys = jax.random.split(jax.random.key(seed), 8)
    return {
        "patches": bell_draw(keys[0], (IMAGES, SEQ, D), 1.0, 6.0, ((0, 8), (1, 16))),
        "weight_codes": touch_ends(jax.random.randint(keys[1], (D, HEADS * HDIM), -448, 449), jax.random.fold_in(keys[1], 1), -448, 448).astype(jnp.int32),
        "block_scales": jnp.clip(jnp.exp(math.log(0.0001) - 1.3862944 * jax.random.uniform(keys[2], (D // BLOCK, HEADS * HDIM // BLOCK), jnp.float32) ** block_scale(keys[2], (D // BLOCK, HEADS * HDIM // BLOCK), ((0, 8),), -0.2, 0.2)), 2.499999936844688e-05, 0.0001),
        "key_proj": bell_draw(keys[3], (IMAGES, SEQ, HEADS * HDIM), 1.0, 6.0, ((0, 8), (1, 16))),
        "value_proj": bell_draw(keys[4], (IMAGES, SEQ, HEADS * HDIM), 1.0, 6.0, ((0, 8), (1, 16))),
        "query_gain": draw_query_gain(jax.random.fold_in(keys[7], 71), 0),
        "key_gain": draw_key_gain(jax.random.fold_in(keys[7], 71), 0),
    }


NORM_FLOOR = 0.25

def head_norm(projected, gain_row):
    shaped = projected.reshape(projected.shape[:-1] + (HEADS, HDIM))
    average = lax.optimization_barrier(jnp.mean(shaped, axis=-1, keepdims=True))
    centred = shaped - average
    spread = lax.optimization_barrier(jnp.mean(centred * centred, axis=-1, keepdims=True))
    normed = centred * lax.rsqrt(spread + NORM_FLOOR) * gain_row.reshape(HEADS, HDIM)
    return normed.astype(jnp.bfloat16)

def reference(patches, weight_codes, block_scales, key_proj, value_proj, query_gain, key_gain):
    column_count = HEADS * HDIM
    blocked = weight_codes.astype(jnp.float32).reshape(D // BLOCK, BLOCK, column_count // BLOCK, BLOCK)
    weight = (blocked * block_scales[:, None, :, None]).reshape(D, column_count).astype(jnp.bfloat16)
    queries = jnp.dot(patches.reshape(IMAGES * SEQ, D), weight, preferred_element_type=jnp.float32)
    queries = queries.reshape(IMAGES, SEQ, column_count)
    query_view = head_norm(queries, query_gain)
    key_view = head_norm(key_proj.astype(jnp.float32), key_gain)
    value_view = value_proj.reshape(IMAGES, SEQ, HEADS, HDIM)

    def one_head(members):
        query_head, key_head, value_head = members
        scores = jnp.einsum('iqd,ikd->iqk', query_head.astype(jnp.float32), key_head.astype(jnp.float32)) * HDIM ** (-0.5)
        largest = lax.optimization_barrier(jnp.max(scores, axis=-1, keepdims=True))
        probability = jnp.exp(scores - largest)
        normaliser = lax.optimization_barrier(jnp.sum(probability, axis=-1))
        rounded = lax.optimization_barrier(probability.astype(jnp.bfloat16))
        blended = jnp.einsum('iqk,ikd->iqd', rounded.astype(jnp.float32), value_head.astype(jnp.float32))
        return blended / normaliser[..., None]
    outputs = lax.map(one_head, (jnp.moveaxis(query_view, 2, 0), jnp.moveaxis(key_view, 2, 0), jnp.moveaxis(value_view, 2, 0)))
    return jnp.moveaxis(outputs, 0, 2).reshape(IMAGES, SEQ, column_count).astype(jnp.bfloat16)
```

```python
import jax
import jax.numpy as jnp
from jax import lax
from jax.experimental import pallas as pl
from jax.experimental.pallas import tpu as pltpu
from jax.sharding import Mesh
from jax.sharding import PartitionSpec as P

HDIM = 64
BLOCK = 128
NORM_FLOOR = 0.25
AXES = ("z", "yh", "c", "yl", "x")
MESH = pl.DeviceIdType.MESH

TOKENS = 128
FEATURES = 3072
ROWS = 384
PAIRS = 3
COLS = PAIRS * BLOCK
HALF = TOKENS // 2

KV_ROUTES = ((0, 1), (1, 0), (1, 1), (3, 0), (3, 1), (2, 0), (2, 1))
X_ROUTES = (1, 3, 2)


def split_dot(values, ones):
    high = values.astype(jnp.bfloat16)
    low = (values - high.astype(jnp.float32)).astype(jnp.bfloat16)
    return jnp.dot(high, ones, preferred_element_type=jnp.float32) + jnp.dot(
        low, ones, preferred_element_type=jnp.float32
    )


def head_ones():
    row = lax.broadcasted_iota(jnp.int32, (BLOCK, BLOCK), 0) // HDIM
    column = lax.broadcasted_iota(jnp.int32, (BLOCK, BLOCK), 1) // HDIM
    return jnp.where(row == column, 1.0, 0.0).astype(jnp.bfloat16)


def pair_norm(values, total, gain_row, ones):
    centred = values - total * (1.0 / HDIM)
    spread = split_dot(centred * centred, ones) * (1.0 / HDIM)
    return centred * lax.rsqrt(spread + NORM_FLOOR) * gain_row


def kernel(
    patches, codes, scales, keys, values, query_gain, key_gain, out,
    patch_all, weight_all, own_kv, kv_all, code_block, query_all, attended,
    local_sem, w_send, w_recv, kv_send, kv_recv, y_send, y_recv, p_send, p_recv, o_send, o_recv, o_local,
):
    z, yh, c = lax.axis_index("z"), lax.axis_index("yh"), lax.axis_index("c")
    yl, x = lax.axis_index("yl"), lax.axis_index("x")
    y = yh * 2 + yl

    def at(dz=0, dy=0, dx=0, dc=0):
        row = lax.rem(y + dy, 4)
        return (
            lax.rem(z + dz, 4), lax.div(row, 2), lax.rem(c + dc, 2), lax.rem(row, 2), lax.rem(x + dx, 4),
        )

    def remote(source, target, send, recv, device):
        return pltpu.make_async_remote_copy(
            src_ref=source, dst_ref=target, send_sem=send, recv_sem=recv, device_id=device, device_id_type=MESH,
        )

    own = z * 2 + c
    chunk = yl * 4 + x
    other_chunk = (1 - yl) * 4 + x
    first_column = pl.multiple_of(own * COLS, BLOCK)

    barrier = pltpu.get_barrier_semaphore()
    partners = [at(dz=dz, dc=dc) for dz, dc in KV_ROUTES]
    partners += [at(dy=dy) for dy in (1, 2, 3)] + [at(dx=dx) for dx in X_ROUTES]
    for partner in partners:
        pl.semaphore_signal(barrier, inc=1, device_id=partner, device_id_type=MESH)

    load_codes = pltpu.make_async_copy(codes.at[:, pl.ds(first_column, COLS)], code_block, local_sem.at[0])
    load_keys = pltpu.make_async_copy(keys.at[0], own_kv.at[0], local_sem.at[1])
    load_values = pltpu.make_async_copy(values.at[0], own_kv.at[1], local_sem.at[2])
    load_patches = pltpu.make_async_copy(patches.at[0], patch_all.at[own], local_sem.at[3])
    for load in (load_codes, load_keys, load_values, load_patches):
        load.start()

    load_codes.wait()
    for r in range(ROWS // BLOCK):
        for k in range(PAIRS):
            block = code_block[r * BLOCK : (r + 1) * BLOCK, k * BLOCK : (k + 1) * BLOCK]
            weight_all[chunk, r * BLOCK : (r + 1) * BLOCK, k * BLOCK : (k + 1) * BLOCK] = (
                block.astype(jnp.float32) * scales[r, own * PAIRS + k]
            ).astype(jnp.bfloat16)
    pl.semaphore_wait(barrier, len(partners))

    half_rows = ROWS // 2
    weight_y = [
        remote(
            weight_all.at[chunk, pl.ds(part * half_rows, half_rows)],
            weight_all.at[chunk, pl.ds(part * half_rows, half_rows)],
            w_send.at[part], w_recv.at[part], at(dy=dy),
        )
        for part, dy in ((0, 1), (1, 3))
    ]
    weight_x = [
        remote(weight_all.at[chunk], weight_all.at[chunk], w_send.at[2 + i], w_recv.at[2 + i], at(dx=dx))
        for i, dx in enumerate(X_ROUTES)
    ]
    weight_x2 = [
        remote(
            weight_all.at[other_chunk], weight_all.at[other_chunk], w_send.at[5 + i], w_recv.at[5 + i], at(dx=dx),
        )
        for i, dx in enumerate(X_ROUTES)
    ]
    for copy in weight_y + weight_x:
        copy.start()

    ones = head_ones()
    load_keys.wait()

    def normalize_keys(k, carry):
        lanes = pl.ds(pl.multiple_of(k * BLOCK, BLOCK), BLOCK)
        block = own_kv[0, :, lanes]
        total = jnp.dot(block, ones, preferred_element_type=jnp.float32)
        own_kv[0, :, lanes] = pair_norm(
            block.astype(jnp.float32), total, key_gain[:, lanes], ones
        ).astype(jnp.bfloat16)
        return carry

    lax.fori_loop(0, FEATURES // BLOCK, normalize_keys, 0, unroll=4)
    load_values.wait()

    def kv_copy(pair, route):
        dz, dc = KV_ROUTES[route]
        target = at(dz=dz, dc=dc)
        column = pl.multiple_of((target[0] * 2 + target[2]) * COLS + pair * BLOCK, BLOCK)
        return remote(
            own_kv.at[:, :, pl.ds(column, BLOCK)], kv_all.at[pair, :, yh, own],
            kv_send.at[pair, route], kv_recv.at[pair, route], target,
        )

    def slot_of(route):
        if route == len(KV_ROUTES):
            return own
        dz, dc = KV_ROUTES[route]
        return lax.rem(z + 4 - dz, 4) * 2 + lax.rem(c + dc, 2)

    def y_copy(pair, route):
        place = kv_all.at[pair, :, yh, slot_of(route)]
        return remote(place, place, y_send.at[pair, route], y_recv.at[pair, route], at(dy=2))

    for pair in range(PAIRS):
        for route in range(len(KV_ROUTES)):
            kv_copy(pair, route).start()

    load_patches.wait()
    low, high = pl.ds(0, HALF), pl.ds(HALF, HALF)
    down, up, across = lax.rem(z + 3, 4) * 2 + c, lax.rem(z + 1, 4) * 2 + c, lax.rem(z + 2, 4) * 2 + c

    def patch_copy(which):
        slot, rows, target = (
            (own, low, at(dz=1)), (own, high, at(dz=1)), (own, high, at(dz=3)), (own, low, at(dz=3)),
            (down, low, at(dz=1)), (up, high, at(dz=3)),
            (own, None, at(dc=1)), (down, None, at(dc=1)), (up, None, at(dc=1)), (across, None, at(dc=1)),
        )[which]
        place = patch_all.at[slot] if rows is None else patch_all.at[slot, rows]
        return remote(place, place, p_send.at[which], p_recv.at[which], target)

    patch_copy(6).start()
    for which in range(4):
        patch_copy(which).start()

    for pair in range(PAIRS):
        for part in range(2):
            kv_all[pair, part, yh, own] = own_kv[
                part, :, pl.ds(pl.multiple_of(own * COLS + pair * BLOCK, BLOCK), BLOCK)
            ]

    for copy in weight_y:
        copy.wait_recv()
    for copy in weight_x2:
        copy.start()

    for pair in range(PAIRS):
        y_copy(pair, len(KV_ROUTES)).start()
        for route in range(len(KV_ROUTES)):
            kv_copy(pair, route).wait_recv()
            y_copy(pair, route).start()
    patch_copy(0).wait_recv()
    patch_copy(4).start()
    patch_copy(2).wait_recv()
    patch_copy(5).start()
    for copy in weight_x + weight_x2:
        copy.wait_recv()

    def out_copy(step, chip, pair, dc):
        target = (chip, yh, lax.rem(c + dc, 2), yl, x)
        lanes = pl.ds(pl.multiple_of(pair * BLOCK, BLOCK), BLOCK)
        column = pl.multiple_of(own * COLS + pair * BLOCK, BLOCK)
        return remote(
            attended.at[step, lax.rem(c + dc, 2), :, lanes], out.at[0, :, pl.ds(column, BLOCK)],
            o_send.at[step, dc, pair], o_recv.at[step, dc, pair], target,
        )

    def out_own(pair):
        lanes = pl.ds(pl.multiple_of(pair * BLOCK, BLOCK), BLOCK)
        column = pl.multiple_of(own * COLS + pair * BLOCK, BLOCK)
        return pltpu.make_async_copy(
            attended.at[0, c, :, lanes], out.at[0, :, pl.ds(column, BLOCK)], o_local.at[pair]
        )

    def chip_of(step):
        away = jnp.where(step == 1, 3, jnp.where(step == 2, 1, jnp.where(step == 3, 2, 0)))
        return lax.rem(z + away, 4)

    first_head = lax.broadcasted_iota(jnp.int32, (2 * TOKENS, BLOCK), 1) < HDIM

    def one_chip(step, carry):
        chip = chip_of(step)

        @pl.when(step == 0)
        def _():
            patch_copy(6).wait_recv()

        @pl.when(step == 1)
        def _():
            patch_copy(1).wait_recv()
            patch_copy(7).start()
            patch_copy(3).wait_recv()
            patch_copy(8).start()
            patch_copy(7).wait_recv()

        @pl.when(step == 2)
        def _():
            patch_copy(8).wait_recv()
            patch_copy(4).wait_recv()
            patch_copy(5).wait_recv()
            patch_copy(9).start()

        @pl.when(step == 3)
        def _():
            patch_copy(9).wait_recv()

        rows = patch_all[pl.ds(chip * 2, 2)].reshape(2 * TOKENS, FEATURES)
        weight = weight_all[...].reshape(FEATURES, COLS)
        queries = jnp.dot(rows, weight, preferred_element_type=jnp.float32)
        for pair in range(PAIRS):
            block = queries[:, pair * BLOCK : (pair + 1) * BLOCK]
            gain = query_gain[:, pl.ds(pl.multiple_of(own * COLS + pair * BLOCK, BLOCK), BLOCK)]
            normed = pair_norm(block, split_dot(block, ones), gain, ones).astype(jnp.bfloat16)
            query_all[pair] = normed * jnp.bfloat16(0.125)

        def one_pair(pair, inner):
            @pl.when(step == 0)
            def _():
                for route in range(len(KV_ROUTES) + 1):
                    y_copy(pair, route).wait_recv()

            query = query_all[pair]
            key = kv_all[pair, 0].reshape(16 * TOKENS, BLOCK)
            value = kv_all[pair, 1].reshape(16 * TOKENS, BLOCK)
            halves = []
            for head in range(2):
                mine = first_head if head == 0 else jnp.logical_not(first_head)
                masked = jnp.where(mine, query, jnp.zeros_like(query))
                scores = lax.dot_general(
                    masked, key, (((1,), (1,)), ((), ())), preferred_element_type=jnp.float32
                )
                largest = jnp.max(scores, axis=1, keepdims=True)
                probability = jnp.exp(scores - largest)
                normaliser = jnp.sum(probability, axis=1, keepdims=True)
                blended = jnp.dot(
                    probability.astype(jnp.bfloat16), value, preferred_element_type=jnp.float32
                )
                halves.append(blended / normaliser)
            mixed = jnp.where(first_head, halves[0], halves[1]).astype(jnp.bfloat16)
            lanes = pl.ds(pl.multiple_of(pair * BLOCK, BLOCK), BLOCK)
            attended[step, :, :, lanes] = mixed.reshape(2, TOKENS, BLOCK)
            out_copy(step, chip, pair, 1).start()

            @pl.when(step == 0)
            def _():
                out_own(pair).start()

            @pl.when(step > 0)
            def _():
                out_copy(step, chip, pair, 0).start()

            return inner

        lax.fori_loop(0, PAIRS, one_pair, 0)
        return carry

    lax.fori_loop(0, 4, one_chip, 0)

    for copy in weight_y + weight_x + weight_x2:
        copy.wait_send()
    for pair in range(PAIRS):
        for route in range(len(KV_ROUTES)):
            kv_copy(pair, route).wait_send()
        for route in range(len(KV_ROUTES) + 1):
            y_copy(pair, route).wait_send()
    for which in range(10):
        patch_copy(which).wait_send()

    def finish(step, carry):
        chip = chip_of(step)
        for pair in range(PAIRS):
            out_copy(step, chip, pair, 1).wait()

            @pl.when(step == 0)
            def _():
                out_own(pair).wait()

            @pl.when(step > 0)
            def _():
                out_copy(step, chip, pair, 0).wait()

        return carry

    lax.fori_loop(0, 4, finish, 0)


def per_device(patches, weight_codes, block_scales, key_proj, value_proj, query_gain, key_gain):
    bf16 = jnp.bfloat16
    dma = pltpu.SemaphoreType.DMA
    anywhere = pl.BlockSpec(memory_space=pl.ANY)
    in_vmem = pl.BlockSpec(memory_space=pltpu.VMEM)
    return pl.pallas_call(
        kernel,
        out_shape=jax.ShapeDtypeStruct((1, TOKENS, FEATURES), bf16),
        in_specs=[
            anywhere, anywhere, pl.BlockSpec(memory_space=pltpu.SMEM), anywhere, anywhere, in_vmem, in_vmem,
        ],
        out_specs=anywhere,
        scratch_shapes=[
            pltpu.VMEM((8, TOKENS, FEATURES), bf16),
            pltpu.VMEM((8, ROWS, COLS), bf16),
            pltpu.VMEM((2, TOKENS, FEATURES), bf16),
            pltpu.VMEM((PAIRS, 2, 2, 8, TOKENS, BLOCK), bf16),
            pltpu.VMEM((ROWS, COLS), jnp.int32),
            pltpu.VMEM((PAIRS, 2 * TOKENS, BLOCK), bf16),
            pltpu.VMEM((4, 2, TOKENS, COLS), bf16),
            dma((4,)), dma((8,)), dma((8,)), dma((PAIRS, 7)), dma((PAIRS, 7)), dma((PAIRS, 8)), dma((PAIRS, 8)),
            dma((10,)), dma((10,)), dma((4, 2, PAIRS)), dma((4, 2, PAIRS)), dma((PAIRS,)),
        ],
        compiler_params=pltpu.CompilerParams(
            collective_id=0, has_side_effects=True, vmem_limit_bytes=60 * 1024 * 1024
        ),
        name="project_attend",
    )(
        patches, weight_codes, block_scales, key_proj, value_proj,
        query_gain.reshape(1, FEATURES), key_gain.reshape(1, FEATURES),
    )


def solution(mesh):
    grid = Mesh(mesh.devices.reshape(4, 2, 2, 2, 4), AXES)
    seq, fsdp = ("z", "yh", "c"), ("yl", "x")
    placed = (
        P(fsdp, seq, None), P(fsdp, None), P(fsdp, None), P(fsdp, seq, None), P(fsdp, seq, None), P(), P(),
    )
    return jax.shard_map(
        per_device, mesh=grid, in_specs=placed, out_specs=P(fsdp, seq, None), check_vma=False
    )
```

```python
import jax
import jax.numpy as jnp
from jax import lax
from jax.experimental import pallas as pl
from jax.experimental.pallas import tpu as pltpu
from jax.sharding import Mesh
from jax.sharding import PartitionSpec as P

HDIM = 64
BLOCK = 128
NORM_FLOOR = 0.25
AXES = ("z", "yh", "c", "yl", "x")
MESH = pl.DeviceIdType.MESH

TOKENS = 128
FEATURES = 3072
ROWS = 384
PAIRS = 3
COLS = PAIRS * BLOCK
HALF = TOKENS // 2
KEYS = 16 * TOKENS
PIECE = 256

KV_ROUTES = ((0, 1), (1, 0), (1, 1), (3, 0), (3, 1), (2, 0), (2, 1))


def split_dot(values, ones):
    high = values.astype(jnp.bfloat16)
    low = (values - high.astype(jnp.float32)).astype(jnp.bfloat16)
    return jnp.dot(high, ones, preferred_element_type=jnp.float32) + jnp.dot(
        low, ones, preferred_element_type=jnp.float32
    )


def head_ones():
    row = lax.broadcasted_iota(jnp.int32, (BLOCK, BLOCK), 0) // HDIM
    column = lax.broadcasted_iota(jnp.int32, (BLOCK, BLOCK), 1) // HDIM
    return jnp.where(row == column, 1.0, 0.0).astype(jnp.bfloat16)


def pair_norm(values, total, gain_row, ones):
    centred = values - total * (1.0 / HDIM)
    spread = split_dot(centred * centred, ones) * (1.0 / HDIM)
    return centred * lax.rsqrt(spread + NORM_FLOOR) * gain_row


def kernel(
    patches, codes, scales, keys, values, query_gain, key_gain, out,
    patch_all, weight_all, own_kv, kv_all, code_block, query_all, attended,
    value_rows, scores_a, scores_b, largest_a, largest_b, blended_a,
    local_sem, w_send, w_recv, kv_send, kv_recv, y_send, y_recv, p_send, p_recv, o_send, o_recv,
):
    z, yh, c = lax.axis_index("z"), lax.axis_index("yh"), lax.axis_index("c")
    yl, x = lax.axis_index("yl"), lax.axis_index("x")
    y = yh * 2 + yl

    def at(dz=0, dy=0, dx=0, dc=0):
        row = lax.rem(y + dy, 4)
        return (
            lax.rem(z + dz, 4), lax.div(row, 2), lax.rem(c + dc, 2), lax.rem(row, 2), lax.rem(x + dx, 4),
        )

    def remote(source, target, send, recv, device):
        return pltpu.make_async_remote_copy(
            src_ref=source, dst_ref=target, send_sem=send, recv_sem=recv, device_id=device, device_id_type=MESH,
        )

    own = z * 2 + c
    chunk = yl * 4 + x
    first_column = pl.multiple_of(own * COLS, BLOCK)

    barrier = pltpu.get_barrier_semaphore()
    partners = [at(dz=dz, dc=dc) for dz, dc in KV_ROUTES]
    partners += [at(dy=dy) for dy in (1, 2, 3)] + [at(dx=dx) for dx in (1, 3)]
    for partner in partners:
        pl.semaphore_signal(barrier, inc=1, device_id=partner, device_id_type=MESH)

    load_codes = pltpu.make_async_copy(codes.at[:, pl.ds(first_column, COLS)], code_block, local_sem.at[0])
    load_keys = pltpu.make_async_copy(keys.at[0], own_kv.at[0], local_sem.at[1])
    load_values = pltpu.make_async_copy(values.at[0], own_kv.at[1], local_sem.at[2])
    load_patches = [
        pltpu.make_async_copy(
            patches.at[0, pl.ds(half * HALF, HALF)], patch_all.at[z, c, half], local_sem.at[3 + half]
        )
        for half in range(2)
    ]
    for load in [load_values, load_codes, load_keys] + load_patches:
        load.start()

    load_codes.wait()
    for r in range(ROWS // BLOCK):
        for k in range(PAIRS):
            block = code_block[r * BLOCK : (r + 1) * BLOCK, k * BLOCK : (k + 1) * BLOCK]
            weight_all[chunk, r * BLOCK : (r + 1) * BLOCK, k * BLOCK : (k + 1) * BLOCK] = (
                block.astype(jnp.float32) * scales[r, own * PAIRS + k]
            ).astype(jnp.bfloat16)

    half_rows = ROWS // 2
    def weight_copy(which):
        low, high = (0, half_rows), (half_rows, half_rows)
        before, after = lax.rem(x + 3, 4), lax.rem(x + 1, 4)
        row, place, rows, target = (
            (yl, x, low, at(dy=1)), (yl, x, high, at(dy=3)),
            (yl, x, None, at(dx=1)), (yl, x, None, at(dx=3)),
            (1 - yl, x, None, at(dx=1)), (1 - yl, x, None, at(dx=3)),
            (yl, before, low, at(dx=1)), (yl, after, high, at(dx=3)),
            (1 - yl, before, low, at(dx=1)), (1 - yl, after, high, at(dx=3)),
        )[which]
        block = weight_all.at[row * 4 + place]
        if rows is not None:
            block = weight_all.at[row * 4 + place, pl.ds(*rows)]
        return remote(block, block, w_send.at[which], w_recv.at[which], target)

    routes = len(KV_ROUTES)

    def kv_copy(part, pair, route):
        dz, dc = KV_ROUTES[route]
        target = at(dz=dz, dc=dc)
        column = pl.multiple_of((target[0] * 2 + target[2]) * COLS + pair * BLOCK, BLOCK)
        return remote(
            own_kv.at[part, :, pl.ds(column, BLOCK)], kv_all.at[pair, part, yh, own],
            kv_send.at[part, pair, route], kv_recv.at[part, pair, route], target,
        )

    def slot_of(route):
        if route == routes:
            return own
        dz, dc = KV_ROUTES[route]
        return lax.rem(z + 4 - dz, 4) * 2 + lax.rem(c + dc, 2)

    def y_copy(part, pair, route):
        place = kv_all.at[pair, part, yh, slot_of(route)]
        return remote(place, place, y_send.at[part, pair, route], y_recv.at[part, pair, route], at(dy=2))

    def send_kv(part, pair):
        for route in range(routes):
            kv_copy(part, pair, route).start()
        column = pl.multiple_of(own * COLS + pair * BLOCK, BLOCK)
        kv_all[pair, part, yh, own] = own_kv[part, :, pl.ds(column, BLOCK)]

    def forward_kv(part, pair):
        y_copy(part, pair, routes).start()
        for route in range(routes):
            kv_copy(part, pair, route).wait_recv()
            y_copy(part, pair, route).start()

    down, up, across = lax.rem(z + 3, 4), lax.rem(z + 1, 4), lax.rem(z + 2, 4)

    def patch_copy(which):
        place, target = (
            ((z, c, 0), at(dz=1)), ((z, c, 1), at(dz=3)), ((z, c, 1), at(dz=1)), ((z, c, 0), at(dz=3)),
            ((down, c, 0), at(dz=1)), ((up, c, 1), at(dz=3)),
            ((z, c), at(dc=1)), ((down, c, 0), at(dc=1)), ((up, c, 1), at(dc=1)),
            ((down, c, 1), at(dc=1)), ((up, c, 0), at(dc=1)),
            ((across, c, 0), at(dc=1)), ((across, c, 1), at(dc=1)),
        )[which]
        block = patch_all.at[place]
        return remote(block, block, p_send.at[which], p_recv.at[which], target)

    ones = head_ones()

    def normalize_keys(pair):
        for owner in range(8):
            lanes = slice((owner * PAIRS + pair) * BLOCK, (owner * PAIRS + pair + 1) * BLOCK)
            block = own_kv[0, :, lanes]
            total = jnp.dot(block, ones, preferred_element_type=jnp.float32)
            own_kv[0, :, lanes] = pair_norm(
                block.astype(jnp.float32), total, key_gain[:, lanes], ones
            ).astype(jnp.bfloat16)

    def forward_weight(first):
        for which in (first, first + 1):
            weight_copy(which).wait_recv()
            weight_copy(which + 4).start()

    load_keys.wait()
    normalize_keys(0)
    load_values.wait()
    for load in load_patches:
        load.wait()
    pl.semaphore_wait(barrier, len(partners))
    for which in range(4):
        weight_copy(which).start()
    patch_copy(6).start()
    send_kv(1, 0)
    send_kv(0, 0)
    normalize_keys(1)
    send_kv(1, 1)
    send_kv(0, 1)
    for which in (0, 1):
        patch_copy(which).start()
    normalize_keys(2)
    send_kv(1, 2)
    send_kv(0, 2)
    for which in (2, 3):
        patch_copy(which).start()
    for which in range(2):
        weight_copy(which).wait_recv()
    for which in range(4, 6):
        weight_copy(which).start()
    forward_kv(1, 0)
    forward_kv(0, 0)
    forward_weight(2)
    forward_kv(1, 1)
    forward_kv(0, 1)
    forward_weight(4)
    for which in range(6, 10):
        weight_copy(which).wait_recv()

    def piece_of(group, k):
        beside = down if k == 0 else up
        chip = jnp.where(group == 0, z, jnp.where(group == 3, across, beside))
        half = jnp.where(group == 2, 1 - k, k)
        return chip, half

    def out_copy(group, pair, dc, k):
        chip, half = piece_of(group, k)
        target = (chip, yh, lax.rem(c + dc, 2), yl, x)
        lanes = pl.ds(pl.multiple_of(pair * BLOCK, BLOCK), BLOCK)
        column = pl.multiple_of(own * COLS + pair * BLOCK, BLOCK)
        rows = pl.ds(pl.multiple_of(half * HALF, HALF), HALF)
        return remote(
            attended.at[group, dc, k, :, lanes], out.at[0, rows, pl.ds(column, BLOCK)],
            o_send.at[group, pair, dc, k], o_recv.at[group, pair, dc, k], target,
        )

    def out_own(pair, k):
        lanes = pl.ds(pl.multiple_of(pair * BLOCK, BLOCK), BLOCK)
        column = pl.multiple_of(own * COLS + pair * BLOCK, BLOCK)
        return pltpu.make_async_copy(
            attended.at[0, 0, k, :, lanes], out.at[0, pl.ds(k * HALF, HALF), pl.ds(column, BLOCK)],
            o_send.at[0, pair, 0, k],
        )

    first_head = lax.broadcasted_iota(jnp.int32, (2 * TOKENS, BLOCK), 1) < HDIM

    def project(group):
        pieces = []
        for dc in range(2):
            for k in range(2):
                chip, half = piece_of(group, k)
                pieces.append(patch_all[chip, lax.rem(c + dc, 2), half])
        rows = jnp.concatenate(pieces, axis=0)
        weight = weight_all[...].reshape(FEATURES, COLS)
        queries = jnp.dot(rows, weight, preferred_element_type=jnp.float32)
        for pair in range(PAIRS):
            block = queries[:, pair * BLOCK : (pair + 1) * BLOCK]
            gain = query_gain[:, pl.ds(pl.multiple_of(own * COLS + pair * BLOCK, BLOCK), BLOCK)]
            normed = pair_norm(block, split_dot(block, ones), gain, ones).astype(jnp.bfloat16)
            normed = normed * jnp.bfloat16(0.125)
            query_all[group, pair, 0] = jnp.where(first_head, normed, jnp.zeros_like(normed))
            query_all[group, pair, 1] = jnp.where(first_head, jnp.zeros_like(normed), normed)

    def group_of(task):
        return jnp.where(task < 4, lax.rem(task, 2), jnp.where(task < 6, 2, jnp.where(task < 9, task - 6, 3)))

    def pair_of(task):
        return jnp.where(task < 4, lax.div(task, 2), jnp.where(task < 6, task - 4, jnp.where(task < 9, 2, task - 9)))

    def any_of(task, *which):
        found = task == which[0]
        for other in which[1:]:
            found = jnp.logical_or(found, task == other)
        return found

    def prepare(task):
        @pl.when(task == 0)
        def _():
            patch_copy(6).wait_recv()

        @pl.when(task == 1)
        def _():
            for which in (0, 1):
                patch_copy(which).wait_recv()
                patch_copy(which + 4).start()
                patch_copy(which + 7).start()
            for which in (7, 8):
                patch_copy(which).wait_recv()

        @pl.when(task == 2)
        def _():
            forward_kv(1, 2)

        @pl.when(task == 3)
        def _():
            forward_kv(0, 2)

        @pl.when(task == 4)
        def _():
            for which in (2, 3):
                patch_copy(which).wait_recv()
                patch_copy(which + 7).start()
            for which in (9, 10):
                patch_copy(which).wait_recv()

        @pl.when(task == 8)
        def _():
            for which in (4, 5):
                patch_copy(which).wait_recv()
                patch_copy(which + 7).start()

        @pl.when(task == 9)
        def _():
            for which in (11, 12):
                patch_copy(which).wait_recv()

        @pl.when(any_of(task, 0, 1, 4, 9))
        def _():
            project(group_of(task))

        @pl.when(any_of(task, 0, 2, 6))
        def _():
            pair = pair_of(task)
            for part in (1, 0):
                for route in range(routes + 1):
                    y_copy(part, pair, route).wait_recv()
            value_rows[pair] = kv_all[pair, 1].reshape(KEYS, BLOCK).T

    def score_piece(task, head, piece, held):
        key = kv_all[pair_of(task), 0, piece // 4, piece % 4 * 2 : piece % 4 * 2 + 2].reshape(PIECE, BLOCK)
        scores = lax.dot_general(
            key, query_all[group_of(task), pair_of(task), head], (((1,), (1,)), ((), ())),
            preferred_element_type=jnp.float32,
        )
        held[piece * PIECE : (piece + 1) * PIECE] = scores
        return jnp.max(scores, axis=0, keepdims=True)

    def blend_piece(task, head, piece, held, largest):
        probability = jnp.exp(held[piece * PIECE : (piece + 1) * PIECE] - largest)
        value = value_rows[
            pair_of(task), head * HDIM : (head + 1) * HDIM, piece * PIECE : (piece + 1) * PIECE
        ]
        return jnp.dot(
            value, probability.astype(jnp.bfloat16), preferred_element_type=jnp.float32
        ), jnp.sum(probability, axis=0, keepdims=True)

    def stage(done_task, done_head, held, largest_ref, next_task, next_head, next_held, next_largest_ref):
        largest = largest_ref[...]
        best = blended = total = None
        for piece in range(KEYS // PIECE):
            tops = score_piece(next_task, next_head, piece, next_held)
            product, part = blend_piece(done_task, done_head, piece, held, largest)
            best = tops if piece == 0 else jnp.maximum(best, tops)
            blended = product if piece == 0 else blended + product
            total = part if piece == 0 else total + part
        next_largest_ref[...] = best
        return blended / total

    prepare(0)
    best = None
    for piece in range(KEYS // PIECE):
        tops = score_piece(0, 0, piece, scores_a)
        best = tops if piece == 0 else jnp.maximum(best, tops)
    largest_a[...] = best

    def one_task(task, carry):
        following = jnp.minimum(task + 1, 4 * PAIRS - 1)
        blended_a[...] = stage(task, 0, scores_a, largest_a, task, 1, scores_b, largest_b)

        @pl.when(task < 4 * PAIRS - 1)
        def _():
            prepare(task + 1)

        second = stage(task, 1, scores_b, largest_b, following, 0, scores_a, largest_a)
        mixed = jnp.concatenate([blended_a[...], second], axis=0).T.astype(jnp.bfloat16)
        group, pair = group_of(task), pair_of(task)
        lanes = pl.ds(pl.multiple_of(pair * BLOCK, BLOCK), BLOCK)
        attended[group, :, :, :, lanes] = mixed.reshape(2, 2, HALF, BLOCK)
        @pl.when(group == 0)
        def _():
            for k in range(2):
                out_copy(group, pair, 1, k).start()
                out_own(pair, k).start()

        @pl.when(task == 7)
        def _():
            for held_group, held_pair in ((1, 0), (1, 1), (2, 0), (2, 1), (1, 2)):
                for dc in range(2):
                    for k in range(2):
                        out_copy(held_group, held_pair, dc, k).start()

        @pl.when(task >= 8)
        def _():
            for dc in range(2):
                for k in range(2):
                    out_copy(group, pair, dc, k).start()

        return carry

    lax.fori_loop(0, 4 * PAIRS, one_task, 0)

    for which in range(10):
        weight_copy(which).wait_send()
    for part in range(2):
        for pair in range(PAIRS):
            for route in range(routes):
                kv_copy(part, pair, route).wait_send()
            for route in range(routes + 1):
                y_copy(part, pair, route).wait_send()
    for which in range(13):
        patch_copy(which).wait_send()

    def finish(group, carry):
        for pair in range(PAIRS):
            for k in range(2):
                out_copy(group, pair, 1, k).wait()

                @pl.when(group == 0)
                def _():
                    out_own(pair, k).wait()

                @pl.when(group > 0)
                def _():
                    out_copy(group, pair, 0, k).wait()

        return carry

    lax.fori_loop(0, 4, finish, 0)


def per_device(patches, weight_codes, block_scales, key_proj, value_proj, query_gain, key_gain):
    bf16, f32 = jnp.bfloat16, jnp.float32
    dma = pltpu.SemaphoreType.DMA
    anywhere = pl.BlockSpec(memory_space=pl.ANY)
    in_vmem = pl.BlockSpec(memory_space=pltpu.VMEM)
    return pl.pallas_call(
        kernel,
        out_shape=jax.ShapeDtypeStruct((1, TOKENS, FEATURES), bf16),
        in_specs=[
            anywhere, anywhere, pl.BlockSpec(memory_space=pltpu.SMEM), anywhere, anywhere, in_vmem, in_vmem,
        ],
        out_specs=anywhere,
        scratch_shapes=[
            pltpu.VMEM((4, 2, 2, HALF, FEATURES), bf16),
            pltpu.VMEM((8, ROWS, COLS), bf16),
            pltpu.VMEM((2, TOKENS, FEATURES), bf16),
            pltpu.VMEM((PAIRS, 2, 2, 8, TOKENS, BLOCK), bf16),
            pltpu.VMEM((ROWS, COLS), jnp.int32),
            pltpu.VMEM((4, PAIRS, 2, 2 * TOKENS, BLOCK), bf16),
            pltpu.VMEM((4, 2, 2, HALF, COLS), bf16),
            pltpu.VMEM((PAIRS, BLOCK, KEYS), bf16),
            pltpu.VMEM((KEYS, 2 * TOKENS), f32),
            pltpu.VMEM((KEYS, 2 * TOKENS), f32),
            pltpu.VMEM((1, 2 * TOKENS), f32),
            pltpu.VMEM((1, 2 * TOKENS), f32),
            pltpu.VMEM((HDIM, 2 * TOKENS), f32),
            dma((5,)), dma((10,)), dma((10,)), dma((2, PAIRS, 7)), dma((2, PAIRS, 7)), dma((2, PAIRS, 8)),
            dma((2, PAIRS, 8)), dma((13,)), dma((13,)), dma((4, PAIRS, 2, 2)), dma((4, PAIRS, 2, 2)),
        ],
        compiler_params=pltpu.CompilerParams(
            collective_id=0, has_side_effects=True, vmem_limit_bytes=60 * 1024 * 1024
        ),
        name="project_attend",
    )(
        patches, weight_codes, block_scales, key_proj, value_proj,
        query_gain.reshape(1, FEATURES), key_gain.reshape(1, FEATURES),
    )


def solution(mesh):
    grid = Mesh(mesh.devices.reshape(4, 2, 2, 2, 4), AXES)
    seq, fsdp = ("z", "yh", "c"), ("yl", "x")
    placed = (
        P(fsdp, seq, None), P(fsdp, None), P(fsdp, None), P(fsdp, seq, None), P(fsdp, seq, None), P(), P(),
    )
    return jax.shard_map(
        per_device, mesh=grid, in_specs=placed, out_specs=P(fsdp, seq, None), check_vma=False
    )
```

```python
import jax
import jax.numpy as jnp
from jax import lax
from jax.experimental import pallas as pl
from jax.experimental.pallas import tpu as pltpu
from jax.sharding import Mesh
from jax.sharding import PartitionSpec as P

HDIM = 64
BLOCK = 128
NORM_FLOOR = 0.25
AXES = ("z", "yh", "c", "yl", "x")
MESH = pl.DeviceIdType.MESH

TOKENS = 128
FEATURES = 3072
ROWS = 384
PAIRS = 3
COLS = PAIRS * BLOCK
HALF = TOKENS // 2
KEYS = 16 * TOKENS
PIECE = 256

KV_ROUTES = ((0, 1), (1, 0), (1, 1), (3, 0), (3, 1), (2, 0), (2, 1))


def split_dot(values, ones):
    high = values.astype(jnp.bfloat16)
    low = (values - high.astype(jnp.float32)).astype(jnp.bfloat16)
    return jnp.dot(high, ones, preferred_element_type=jnp.float32) + jnp.dot(
        low, ones, preferred_element_type=jnp.float32
    )


def head_ones():
    row = lax.broadcasted_iota(jnp.int32, (BLOCK, BLOCK), 0) // HDIM
    column = lax.broadcasted_iota(jnp.int32, (BLOCK, BLOCK), 1) // HDIM
    return jnp.where(row == column, 1.0, 0.0).astype(jnp.bfloat16)


def pair_norm(values, total, gain_row, ones):
    centred = values - total * (1.0 / HDIM)
    spread = split_dot(centred * centred, ones) * (1.0 / HDIM)
    return centred * lax.rsqrt(spread + NORM_FLOOR) * gain_row


def kernel(
    patches, codes, scales, keys, values, query_gain, key_gain, out,
    patch_all, weight_all, own_kv, kv_all, code_block, query_all, attended,
    value_rows, scores_a, scores_b, largest_a, largest_b, blended_a,
    local_sem, w_send, w_recv, kv_send, kv_recv, y_send, y_recv, p_send, p_recv, o_send, o_recv,
):
    z, yh, c = lax.axis_index("z"), lax.axis_index("yh"), lax.axis_index("c")
    yl, x = lax.axis_index("yl"), lax.axis_index("x")
    y = yh * 2 + yl

    def at(dz=0, dy=0, dx=0, dc=0):
        row = lax.rem(y + dy, 4)
        return (
            lax.rem(z + dz, 4), lax.div(row, 2), lax.rem(c + dc, 2), lax.rem(row, 2), lax.rem(x + dx, 4),
        )

    def remote(source, target, send, recv, device):
        return pltpu.make_async_remote_copy(
            src_ref=source, dst_ref=target, send_sem=send, recv_sem=recv, device_id=device, device_id_type=MESH,
        )

    own = z * 2 + c
    chunk = yl * 4 + x
    first_column = pl.multiple_of(own * COLS, BLOCK)

    barrier = pltpu.get_barrier_semaphore()
    partners = [at(dz=dz, dc=dc) for dz, dc in KV_ROUTES]
    partners += [at(dy=dy) for dy in (1, 2, 3)] + [at(dx=dx) for dx in (1, 3)]
    for partner in partners:
        pl.semaphore_signal(barrier, inc=1, device_id=partner, device_id_type=MESH)

    load_codes = pltpu.make_async_copy(codes.at[:, pl.ds(first_column, COLS)], code_block, local_sem.at[0])
    load_keys = pltpu.make_async_copy(keys.at[0], own_kv.at[0], local_sem.at[1])
    load_values = pltpu.make_async_copy(values.at[0], own_kv.at[1], local_sem.at[2])
    load_patches = [
        pltpu.make_async_copy(
            patches.at[0, pl.ds(half * HALF, HALF)], patch_all.at[z, c, half], local_sem.at[3 + half]
        )
        for half in range(2)
    ]
    for load in [load_values, load_codes, load_keys] + load_patches:
        load.start()

    load_codes.wait()
    for r in range(ROWS // BLOCK):
        for k in range(PAIRS):
            block = code_block[r * BLOCK : (r + 1) * BLOCK, k * BLOCK : (k + 1) * BLOCK]
            weight_all[chunk, r * BLOCK : (r + 1) * BLOCK, k * BLOCK : (k + 1) * BLOCK] = (
                block.astype(jnp.float32) * scales[r, own * PAIRS + k]
            ).astype(jnp.bfloat16)

    half_rows = ROWS // 2
    def weight_copy(which):
        low, high = (0, half_rows), (half_rows, half_rows)
        before, after = lax.rem(x + 3, 4), lax.rem(x + 1, 4)
        row, place, rows, target = (
            (yl, x, low, at(dy=1)), (yl, x, high, at(dy=3)),
            (yl, x, None, at(dx=1)), (yl, x, None, at(dx=3)),
            (1 - yl, x, None, at(dx=1)), (1 - yl, x, None, at(dx=3)),
            (yl, before, low, at(dx=1)), (yl, after, high, at(dx=3)),
            (1 - yl, before, low, at(dx=1)), (1 - yl, after, high, at(dx=3)),
        )[which]
        block = weight_all.at[row * 4 + place]
        if rows is not None:
            block = weight_all.at[row * 4 + place, pl.ds(*rows)]
        return remote(block, block, w_send.at[which], w_recv.at[which], target)

    routes = len(KV_ROUTES)

    def kv_copy(part, pair, route):
        dz, dc = KV_ROUTES[route]
        target = at(dz=dz, dc=dc)
        column = pl.multiple_of((target[0] * 2 + target[2]) * COLS + pair * BLOCK, BLOCK)
        return remote(
            own_kv.at[part, :, pl.ds(column, BLOCK)], kv_all.at[pair, part, yh, own],
            kv_send.at[part, pair, route], kv_recv.at[part, pair, route], target,
        )

    def slot_of(route):
        if route == routes:
            return own
        dz, dc = KV_ROUTES[route]
        return lax.rem(z + 4 - dz, 4) * 2 + lax.rem(c + dc, 2)

    def y_copy(part, pair, route):
        place = kv_all.at[pair, part, yh, slot_of(route)]
        return remote(place, place, y_send.at[part, pair, route], y_recv.at[part, pair, route], at(dy=2))

    def send_kv(part, pair):
        for route in range(routes):
            kv_copy(part, pair, route).start()
        column = pl.multiple_of(own * COLS + pair * BLOCK, BLOCK)
        kv_all[pair, part, yh, own] = own_kv[part, :, pl.ds(column, BLOCK)]
        if pair < 2:
            y_copy(part, pair, routes).start()

    def forward_kv(part, pair):
        if pair == 2:
            y_copy(part, pair, routes).start()
        for route in range(routes):
            kv_copy(part, pair, route).wait_recv()
            y_copy(part, pair, route).start()

    down, up, across = lax.rem(z + 3, 4), lax.rem(z + 1, 4), lax.rem(z + 2, 4)

    def patch_copy(which):
        place, target = (
            ((z, c, 0), at(dz=1)), ((z, c, 1), at(dz=3)), ((z, c, 1), at(dz=1)), ((z, c, 0), at(dz=3)),
            ((down, c, 0), at(dz=1)), ((up, c, 1), at(dz=3)),
            ((z, c), at(dc=1)), ((down, c, 0), at(dc=1)), ((up, c, 1), at(dc=1)),
            ((down, c, 1), at(dc=1)), ((up, c, 0), at(dc=1)),
            ((across, c, 0), at(dc=1)), ((across, c, 1), at(dc=1)),
        )[which]
        block = patch_all.at[place]
        return remote(block, block, p_send.at[which], p_recv.at[which], target)

    ones = head_ones()

    def normalize_keys(pair):
        for owner in range(8):
            lanes = slice((owner * PAIRS + pair) * BLOCK, (owner * PAIRS + pair + 1) * BLOCK)
            block = own_kv[0, :, lanes]
            total = jnp.dot(block, ones, preferred_element_type=jnp.float32)
            own_kv[0, :, lanes] = pair_norm(
                block.astype(jnp.float32), total, key_gain[:, lanes], ones
            ).astype(jnp.bfloat16)

    def forward_weight(first):
        for which in (first, first + 1):
            weight_copy(which).wait_recv()
            weight_copy(which + 4).start()

    load_keys.wait()
    normalize_keys(0)
    load_values.wait()
    for load in load_patches:
        load.wait()
    pl.semaphore_wait(barrier, len(partners))
    for which in range(4):
        weight_copy(which).start()
    patch_copy(6).start()
    send_kv(1, 0)
    send_kv(0, 0)
    normalize_keys(1)
    send_kv(1, 1)
    send_kv(0, 1)
    for which in (0, 1):
        patch_copy(which).start()
    normalize_keys(2)
    send_kv(1, 2)
    send_kv(0, 2)
    for which in (2, 3):
        patch_copy(which).start()
    for which in range(2):
        weight_copy(which).wait_recv()
    for which in range(4, 6):
        weight_copy(which).start()
    forward_kv(1, 0)
    forward_kv(0, 0)
    forward_weight(2)
    forward_kv(1, 1)
    forward_kv(0, 1)
    forward_weight(4)
    for which in range(6, 10):
        weight_copy(which).wait_recv()

    def piece_of(group, k):
        beside = down if k == 0 else up
        chip = jnp.where(group == 0, z, jnp.where(group == 3, across, beside))
        half = jnp.where(group == 2, 1 - k, k)
        return chip, half

    def out_copy(group, pair, dc, k):
        chip, half = piece_of(group, k)
        target = (chip, yh, lax.rem(c + dc, 2), yl, x)
        lanes = pl.ds(pl.multiple_of(pair * BLOCK, BLOCK), BLOCK)
        column = pl.multiple_of(own * COLS + pair * BLOCK, BLOCK)
        rows = pl.ds(pl.multiple_of(half * HALF, HALF), HALF)
        return remote(
            attended.at[group, dc, k, :, lanes], out.at[0, rows, pl.ds(column, BLOCK)],
            o_send.at[group, pair, dc, k], o_recv.at[group, pair, dc, k], target,
        )

    def out_own(pair, k):
        lanes = pl.ds(pl.multiple_of(pair * BLOCK, BLOCK), BLOCK)
        column = pl.multiple_of(own * COLS + pair * BLOCK, BLOCK)
        return pltpu.make_async_copy(
            attended.at[0, 0, k, :, lanes], out.at[0, pl.ds(k * HALF, HALF), pl.ds(column, BLOCK)],
            o_send.at[0, pair, 0, k],
        )

    first_head = lax.broadcasted_iota(jnp.int32, (2 * TOKENS, BLOCK), 1) < HDIM

    def project(group):
        pieces = []
        for dc in range(2):
            for k in range(2):
                chip, half = piece_of(group, k)
                pieces.append(patch_all[chip, lax.rem(c + dc, 2), half])
        rows = jnp.concatenate(pieces, axis=0)
        weight = weight_all[...].reshape(FEATURES, COLS)
        queries = jnp.dot(rows, weight, preferred_element_type=jnp.float32)
        for pair in range(PAIRS):
            block = queries[:, pair * BLOCK : (pair + 1) * BLOCK]
            gain = query_gain[:, pl.ds(pl.multiple_of(own * COLS + pair * BLOCK, BLOCK), BLOCK)]
            normed = pair_norm(block, split_dot(block, ones), gain, ones).astype(jnp.bfloat16)
            normed = normed * jnp.bfloat16(0.125)
            query_all[group, pair, 0] = jnp.where(first_head, normed, jnp.zeros_like(normed))
            query_all[group, pair, 1] = jnp.where(first_head, jnp.zeros_like(normed), normed)

    def any_of(task, *which):
        found = task == which[0]
        for other in which[1:]:
            found = jnp.logical_or(found, task == other)
        return found

    def group_of(task):
        late = jnp.where(task == 6, 2, jnp.where(task == 7, 1, jnp.where(task == 11, 0, 3)))
        return jnp.where(task < 4, lax.rem(task, 2), jnp.where(task < 6, 2, late))

    def pair_of(task):
        late = jnp.where(any_of(task, 8, 9), task - 8, 2)
        return jnp.where(task < 4, lax.div(task, 2), jnp.where(task < 6, task - 4, late))

    def prepare(task):
        @pl.when(task == 0)
        def _():
            patch_copy(6).wait_recv()

        @pl.when(task == 1)
        def _():
            for which in (0, 1):
                patch_copy(which).wait_recv()
                patch_copy(which + 4).start()
                patch_copy(which + 7).start()
            for which in (7, 8):
                patch_copy(which).wait_recv()
            forward_kv(1, 2)

        @pl.when(task == 2)
        def _():
            forward_kv(0, 2)

        @pl.when(task == 4)
        def _():
            for which in (2, 3):
                patch_copy(which).wait_recv()
                patch_copy(which + 7).start()
            for which in (9, 10):
                patch_copy(which).wait_recv()

        @pl.when(task == 8)
        def _():
            for which in (11, 12):
                patch_copy(which).wait_recv()

        @pl.when(any_of(task, 0, 1, 4, 8))
        def _():
            project(group_of(task))

        @pl.when(any_of(task, 0, 2, 6))
        def _():
            pair = pair_of(task)
            for part in (1, 0):
                for route in range(routes + 1):
                    y_copy(part, pair, route).wait_recv()
            value_rows[pair] = kv_all[pair, 1].reshape(KEYS, BLOCK).T

    def score_piece(task, head, piece, held):
        key = kv_all[pair_of(task), 0, piece // 4, piece % 4 * 2 : piece % 4 * 2 + 2].reshape(PIECE, BLOCK)
        scores = lax.dot_general(
            key, query_all[group_of(task), pair_of(task), head], (((1,), (1,)), ((), ())),
            preferred_element_type=jnp.float32,
        )
        held[piece * PIECE : (piece + 1) * PIECE] = scores
        return jnp.max(scores, axis=0, keepdims=True)

    def blend_piece(task, head, piece, held, largest):
        probability = jnp.exp(held[piece * PIECE : (piece + 1) * PIECE] - largest)
        value = value_rows[
            pair_of(task), head * HDIM : (head + 1) * HDIM, piece * PIECE : (piece + 1) * PIECE
        ]
        return jnp.dot(
            value, probability.astype(jnp.bfloat16), preferred_element_type=jnp.float32
        ), jnp.sum(probability, axis=0, keepdims=True)

    def stage(done_task, done_head, held, largest_ref, next_task, next_head, next_held, next_largest_ref):
        largest = largest_ref[...]
        best = blended = total = None
        for piece in range(KEYS // PIECE):
            tops = score_piece(next_task, next_head, piece, next_held)
            product, part = blend_piece(done_task, done_head, piece, held, largest)
            best = tops if piece == 0 else jnp.maximum(best, tops)
            blended = product if piece == 0 else blended + product
            total = part if piece == 0 else total + part
        next_largest_ref[...] = best
        return blended / total

    prepare(0)
    best = None
    for piece in range(KEYS // PIECE):
        tops = score_piece(0, 0, piece, scores_a)
        best = tops if piece == 0 else jnp.maximum(best, tops)
    largest_a[...] = best

    def one_task(task, carry):
        following = jnp.minimum(task + 1, 4 * PAIRS - 1)

        @pl.when(task == 7)
        def _():
            for which in (4, 5):
                patch_copy(which).wait_recv()
                patch_copy(which + 7).start()

        blended_a[...] = stage(task, 0, scores_a, largest_a, task, 1, scores_b, largest_b)

        @pl.when(task < 4 * PAIRS - 1)
        def _():
            prepare(task + 1)

        second = stage(task, 1, scores_b, largest_b, following, 0, scores_a, largest_a)
        mixed = jnp.concatenate([blended_a[...], second], axis=0).T.astype(jnp.bfloat16)
        group, pair = group_of(task), pair_of(task)
        lanes = pl.ds(pl.multiple_of(pair * BLOCK, BLOCK), BLOCK)
        attended[group, :, :, :, lanes] = mixed.reshape(2, 2, HALF, BLOCK)
        @pl.when(group == 0)
        def _():
            for k in range(2):
                out_copy(group, pair, 1, k).start()
                out_own(pair, k).start()

        @pl.when(group > 0)
        def _():
            for dc in range(2):
                for k in range(2):
                    out_copy(group, pair, dc, k).start()

        return carry

    lax.fori_loop(0, 4 * PAIRS, one_task, 0)

    for which in range(10):
        weight_copy(which).wait_send()
    for part in range(2):
        for pair in range(PAIRS):
            for route in range(routes):
                kv_copy(part, pair, route).wait_send()
            for route in range(routes + 1):
                y_copy(part, pair, route).wait_send()
    for which in range(13):
        patch_copy(which).wait_send()

    def finish(group, carry):
        for pair in range(PAIRS):
            for k in range(2):
                out_copy(group, pair, 1, k).wait()

                @pl.when(group == 0)
                def _():
                    out_own(pair, k).wait()

                @pl.when(group > 0)
                def _():
                    out_copy(group, pair, 0, k).wait()

        return carry

    lax.fori_loop(0, 4, finish, 0)


def per_device(patches, weight_codes, block_scales, key_proj, value_proj, query_gain, key_gain):
    bf16, f32 = jnp.bfloat16, jnp.float32
    dma = pltpu.SemaphoreType.DMA
    anywhere = pl.BlockSpec(memory_space=pl.ANY)
    in_vmem = pl.BlockSpec(memory_space=pltpu.VMEM)
    mixed = pl.pallas_call(
        kernel,
        out_shape=jax.ShapeDtypeStruct((1, TOKENS, FEATURES), bf16),
        in_specs=[
            anywhere, anywhere, pl.BlockSpec(memory_space=pltpu.SMEM), anywhere, anywhere, in_vmem, in_vmem,
        ],
        out_specs=anywhere,
        scratch_shapes=[
            pltpu.VMEM((4, 2, 2, HALF, FEATURES), bf16),
            pltpu.VMEM((8, ROWS, COLS), bf16),
            pltpu.VMEM((2, TOKENS, FEATURES), bf16),
            pltpu.VMEM((PAIRS, 2, 2, 8, TOKENS, BLOCK), bf16),
            pltpu.VMEM((ROWS, COLS), jnp.int32),
            pltpu.VMEM((4, PAIRS, 2, 2 * TOKENS, BLOCK), bf16),
            pltpu.VMEM((4, 2, 2, HALF, COLS), bf16),
            pltpu.VMEM((PAIRS, BLOCK, KEYS), bf16),
            pltpu.VMEM((KEYS, 2 * TOKENS), f32),
            pltpu.VMEM((KEYS, 2 * TOKENS), f32),
            pltpu.VMEM((1, 2 * TOKENS), f32),
            pltpu.VMEM((1, 2 * TOKENS), f32),
            pltpu.VMEM((HDIM, 2 * TOKENS), f32),
            dma((5,)), dma((10,)), dma((10,)), dma((2, PAIRS, 7)), dma((2, PAIRS, 7)), dma((2, PAIRS, 8)),
            dma((2, PAIRS, 8)), dma((13,)), dma((13,)), dma((4, PAIRS, 2, 2)), dma((4, PAIRS, 2, 2)),
        ],
        compiler_params=pltpu.CompilerParams(
            collective_id=0, has_side_effects=True, vmem_limit_bytes=60 * 1024 * 1024
        ),
        name="project_attend",
    )(
        patches, weight_codes, block_scales, key_proj, value_proj,
        query_gain.reshape(1, FEATURES), key_gain.reshape(1, FEATURES),
    )
    def place(source, target):
        target[...] = source[...]
    return pl.pallas_call(
        place,
        out_shape=jax.ShapeDtypeStruct((1, TOKENS, FEATURES), bf16),
        grid=(2,),
        in_specs=[pl.BlockSpec((1, TOKENS // 2, FEATURES), lambda i: (0, i, 0))],
        out_specs=pl.BlockSpec((1, TOKENS // 2, FEATURES), lambda i: (0, i, 0)),
        name="place",
    )(mixed)


def solution(mesh):
    grid = Mesh(mesh.devices.reshape(4, 2, 2, 2, 4), AXES)
    seq, fsdp = ("z", "yh", "c"), ("yl", "x")
    placed = (
        P(fsdp, seq, None), P(fsdp, None), P(fsdp, None), P(fsdp, seq, None), P(fsdp, seq, None), P(), P(),
    )
    return jax.shard_map(
        per_device, mesh=grid, in_specs=placed, out_specs=P(fsdp, seq, None), check_vma=False
    )
```

```python
import jax
import jax.numpy as jnp
from jax import lax
from jax.experimental import pallas as pl
from jax.experimental.pallas import tpu as pltpu
from jax.sharding import Mesh
from jax.sharding import PartitionSpec as P

HDIM = 64
BLOCK = 128
NORM_FLOOR = 0.25
AXES = ("z", "yh", "c", "yl", "x")
MESH = pl.DeviceIdType.MESH

TOKENS = 128
FEATURES = 3072
ROWS = 384
PAIRS = 3
COLS = PAIRS * BLOCK
HALF = TOKENS // 2
KEYS = 16 * TOKENS
PIECE = 256
PART = FEATURES // 2

KV_ROUTES = ((0, 1), (1, 0), (1, 1), (3, 0), (3, 1), (2, 0), (2, 1))


def split_dot(values, ones):
    high = values.astype(jnp.bfloat16)
    low = (values - high.astype(jnp.float32)).astype(jnp.bfloat16)
    return jnp.dot(
        jnp.concatenate([high, low], axis=1), jnp.concatenate([ones, ones], axis=0),
        preferred_element_type=jnp.float32,
    )


def head_ones():
    row = lax.broadcasted_iota(jnp.int32, (BLOCK, BLOCK), 0) // HDIM
    column = lax.broadcasted_iota(jnp.int32, (BLOCK, BLOCK), 1) // HDIM
    return jnp.where(row == column, 1.0, 0.0).astype(jnp.bfloat16)


def pair_norm(values, total, gain_row, ones):
    centred = values - total * (1.0 / HDIM)
    spread = split_dot(centred * centred, ones) * (1.0 / HDIM)
    return centred * lax.rsqrt(spread + NORM_FLOOR) * gain_row


def kernel(
    patches, codes, scales, keys, values, query_gain, key_gain, out,
    patch_all, weight_all, own_kv, kv_all, code_block, query_all, attended,
    value_rows, scores_a, scores_b, largest_a, largest_b, blended_a, partial,
    local_sem, w_send, w_recv, kv_send, kv_recv, y_send, y_recv, p_send, p_recv, o_send, o_recv,
):
    z, yh, c = lax.axis_index("z"), lax.axis_index("yh"), lax.axis_index("c")
    yl, x = lax.axis_index("yl"), lax.axis_index("x")
    y = yh * 2 + yl

    def at(dz=0, dy=0, dx=0, dc=0):
        row = lax.rem(y + dy, 4)
        return (
            lax.rem(z + dz, 4), lax.div(row, 2), lax.rem(c + dc, 2), lax.rem(row, 2), lax.rem(x + dx, 4),
        )

    def remote(source, target, send, recv, device):
        return pltpu.make_async_remote_copy(
            src_ref=source, dst_ref=target, send_sem=send, recv_sem=recv, device_id=device, device_id_type=MESH,
        )

    own = z * 2 + c
    chunk = yl * 4 + x
    first_column = pl.multiple_of(own * COLS, BLOCK)

    barrier = pltpu.get_barrier_semaphore()
    partners = [at(dz=dz, dc=dc) for dz, dc in KV_ROUTES]
    partners += [at(dy=dy) for dy in (1, 2, 3)] + [at(dx=dx) for dx in (1, 3)]
    for partner in partners:
        pl.semaphore_signal(barrier, inc=1, device_id=partner, device_id_type=MESH)

    load_codes = pltpu.make_async_copy(codes.at[:, pl.ds(first_column, COLS)], code_block, local_sem.at[0])
    load_keys = pltpu.make_async_copy(keys.at[0], own_kv.at[0], local_sem.at[1])
    load_values = pltpu.make_async_copy(values.at[0], own_kv.at[1], local_sem.at[2])
    load_patches = [
        pltpu.make_async_copy(
            patches.at[0, pl.ds(half * HALF, HALF)], patch_all.at[z, c, half], local_sem.at[3 + half]
        )
        for half in range(2)
    ]
    for load in [load_values, load_codes, load_keys] + load_patches:
        load.start()

    load_codes.wait()
    for r in range(ROWS // BLOCK):
        for k in range(PAIRS):
            block = code_block[r * BLOCK : (r + 1) * BLOCK, k * BLOCK : (k + 1) * BLOCK]
            weight_all[chunk, r * BLOCK : (r + 1) * BLOCK, k * BLOCK : (k + 1) * BLOCK] = (
                block.astype(jnp.float32) * scales[r, own * PAIRS + k]
            ).astype(jnp.bfloat16)

    half_rows = ROWS // 2
    def weight_copy(which):
        low, high = (0, half_rows), (half_rows, half_rows)
        before, after = lax.rem(x + 3, 4), lax.rem(x + 1, 4)
        row, place, rows, target = (
            (yl, x, low, at(dy=1)), (yl, x, high, at(dy=3)),
            (yl, x, None, at(dx=1)), (yl, x, None, at(dx=3)),
            (1 - yl, x, None, at(dx=1)), (1 - yl, x, None, at(dx=3)),
            (yl, before, low, at(dx=1)), (yl, after, high, at(dx=3)),
            (1 - yl, before, low, at(dx=1)), (1 - yl, after, high, at(dx=3)),
        )[which]
        block = weight_all.at[row * 4 + place]
        if rows is not None:
            block = weight_all.at[row * 4 + place, pl.ds(*rows)]
        return remote(block, block, w_send.at[which], w_recv.at[which], target)

    routes = len(KV_ROUTES)

    def kv_copy(part, pair, route):
        dz, dc = KV_ROUTES[route]
        target = at(dz=dz, dc=dc)
        column = pl.multiple_of((target[0] * 2 + target[2]) * COLS + pair * BLOCK, BLOCK)
        return remote(
            own_kv.at[part, :, pl.ds(column, BLOCK)], kv_all.at[pair, part, yh, own],
            kv_send.at[part, pair, route], kv_recv.at[part, pair, route], target,
        )

    def slot_of(route):
        if route == routes:
            return own
        dz, dc = KV_ROUTES[route]
        return lax.rem(z + 4 - dz, 4) * 2 + lax.rem(c + dc, 2)

    def y_copy(part, pair, route):
        place = kv_all.at[pair, part, yh, slot_of(route)]
        return remote(place, place, y_send.at[part, pair, route], y_recv.at[part, pair, route], at(dy=2))

    def send_kv(part, pair):
        for route in range(routes):
            kv_copy(part, pair, route).start()
        column = pl.multiple_of(own * COLS + pair * BLOCK, BLOCK)
        kv_all[pair, part, yh, own] = own_kv[part, :, pl.ds(column, BLOCK)]
        if pair < 2:
            y_copy(part, pair, routes).start()

    def forward_kv(part, pair):
        if pair == 2:
            y_copy(part, pair, routes).start()
        for route in range(routes):
            kv_copy(part, pair, route).wait_recv()
            y_copy(part, pair, route).start()

    down, up, across = lax.rem(z + 3, 4), lax.rem(z + 1, 4), lax.rem(z + 2, 4)

    def patch_copy(which, part):
        place, target = (
            ((z, c, 0), at(dz=1)), ((z, c, 1), at(dz=3)), ((z, c, 1), at(dz=1)), ((z, c, 0), at(dz=3)),
            ((down, c, 0), at(dz=1)), ((up, c, 1), at(dz=3)),
            ((z, c, slice(None)), at(dc=1)), ((down, c, 0), at(dc=1)), ((up, c, 1), at(dc=1)),
            ((down, c, 1), at(dc=1)), ((up, c, 0), at(dc=1)),
            ((across, c, 0), at(dc=1)), ((across, c, 1), at(dc=1)),
        )[which]
        block = patch_all.at[(*place, slice(None), pl.ds(part * PART, PART))]
        return remote(block, block, p_send.at[which, part], p_recv.at[which, part], target)

    ones = head_ones()

    def normalize_keys(pair):
        for owner in range(8):
            lanes = slice((owner * PAIRS + pair) * BLOCK, (owner * PAIRS + pair + 1) * BLOCK)
            block = own_kv[0, :, lanes]
            total = jnp.dot(block, ones, preferred_element_type=jnp.float32)
            own_kv[0, :, lanes] = pair_norm(
                block.astype(jnp.float32), total, key_gain[:, lanes], ones
            ).astype(jnp.bfloat16)

    def forward_weight(first):
        for which in (first, first + 1):
            weight_copy(which).wait_recv()
            weight_copy(which + 4).start()

    load_keys.wait()
    normalize_keys(0)
    load_values.wait()
    for load in load_patches:
        load.wait()
    pl.semaphore_wait(barrier, len(partners))
    for which in range(4):
        weight_copy(which).start()
    for part in range(2):
        patch_copy(6, part).start()
    send_kv(1, 0)
    send_kv(0, 0)
    normalize_keys(1)
    send_kv(1, 1)
    send_kv(0, 1)
    for part in range(2):
        for which in (0, 1):
            patch_copy(which, part).start()
    normalize_keys(2)
    send_kv(1, 2)
    send_kv(0, 2)
    for part in range(2):
        for which in (2, 3):
            patch_copy(which, part).start()
    for which in range(2):
        weight_copy(which).wait_recv()
    for which in range(4, 6):
        weight_copy(which).start()
    forward_kv(1, 0)
    forward_kv(0, 0)
    forward_weight(2)
    forward_kv(1, 1)
    forward_kv(0, 1)
    forward_weight(4)
    for which in range(6, 10):
        weight_copy(which).wait_recv()

    def piece_of(group, k):
        beside = down if k == 0 else up
        chip = jnp.where(group == 0, z, jnp.where(group == 3, across, beside))
        half = jnp.where(group == 2, 1 - k, k)
        return chip, half

    def out_copy(group, pair, dc, k):
        chip, half = piece_of(group, k)
        target = (chip, yh, lax.rem(c + dc, 2), yl, x)
        lanes = pl.ds(pl.multiple_of(pair * BLOCK, BLOCK), BLOCK)
        column = pl.multiple_of(own * COLS + pair * BLOCK, BLOCK)
        rows = pl.ds(pl.multiple_of(half * HALF, HALF), HALF)
        return remote(
            attended.at[group, dc, k, :, lanes], out.at[0, rows, pl.ds(column, BLOCK)],
            o_send.at[group, pair, dc, k], o_recv.at[group, pair, dc, k], target,
        )

    def out_own(pair, k):
        lanes = pl.ds(pl.multiple_of(pair * BLOCK, BLOCK), BLOCK)
        column = pl.multiple_of(own * COLS + pair * BLOCK, BLOCK)
        return pltpu.make_async_copy(
            attended.at[0, 0, k, :, lanes], out.at[0, pl.ds(k * HALF, HALF), pl.ds(column, BLOCK)],
            o_send.at[0, pair, 0, k],
        )

    first_head = lax.broadcasted_iota(jnp.int32, (2 * TOKENS, BLOCK), 1) < HDIM

    def project(group, part):
        pieces = []
        for dc in range(2):
            for k in range(2):
                chip, half = piece_of(group, k)
                pieces.append(patch_all[chip, lax.rem(c + dc, 2), half, :, part * PART : (part + 1) * PART])
        rows = jnp.concatenate(pieces, axis=0)
        weight = weight_all[part * 4 : (part + 1) * 4].reshape(PART, COLS)
        return jnp.dot(rows, weight, preferred_element_type=jnp.float32)

    def normalize_queries(group, queries):
        for pair in range(PAIRS):
            block = queries[:, pair * BLOCK : (pair + 1) * BLOCK]
            gain = query_gain[:, pl.ds(pl.multiple_of(own * COLS + pair * BLOCK, BLOCK), BLOCK)]
            normed = pair_norm(block, split_dot(block, ones), gain, ones).astype(jnp.bfloat16)
            normed = normed * jnp.bfloat16(0.125)
            query_all[group, pair, 0] = jnp.where(first_head, normed, jnp.zeros_like(normed))
            query_all[group, pair, 1] = jnp.where(first_head, jnp.zeros_like(normed), normed)

    def any_of(task, *which):
        found = task == which[0]
        for other in which[1:]:
            found = jnp.logical_or(found, task == other)
        return found

    def group_of(task):
        late = jnp.where(task == 6, 2, jnp.where(task == 7, 1, jnp.where(task == 11, 0, 3)))
        return jnp.where(task < 4, lax.rem(task, 2), jnp.where(task < 6, 2, late))

    def pair_of(task):
        late = jnp.where(any_of(task, 8, 9), task - 8, 2)
        return jnp.where(task < 4, lax.div(task, 2), jnp.where(task < 6, task - 4, late))

    def prepare(task):
        def arrive(*which):
            for part in range(2):
                for other in which:
                    patch_copy(other, part).wait_recv()

        @pl.when(task == 0)
        def _():
            arrive(6)

        @pl.when(task == 1)
        def _():
            for part in range(2):
                for which in (0, 1):
                    patch_copy(which, part).wait_recv()
                    patch_copy(which + 4, part).start()
                    patch_copy(which + 7, part).start()
            arrive(7, 8)
            forward_kv(1, 2)

        @pl.when(task == 2)
        def _():
            forward_kv(0, 2)

        @pl.when(any_of(task, 0, 1, 4, 8))
        def _():
            group = group_of(task)

            @pl.when(task == 4)
            def _():
                for which in (2, 3):
                    patch_copy(which, 0).wait_recv()
                    patch_copy(which + 7, 0).start()
                for which in (9, 10):
                    patch_copy(which, 0).wait_recv()

            @pl.when(task == 8)
            def _():
                for which in (11, 12):
                    patch_copy(which, 0).wait_recv()

            partial[...] = project(group, 0)

            @pl.when(task == 4)
            def _():
                for which in (2, 3):
                    patch_copy(which, 1).wait_recv()
                    patch_copy(which + 7, 1).start()
                for which in (9, 10):
                    patch_copy(which, 1).wait_recv()

            @pl.when(task == 8)
            def _():
                for which in (11, 12):
                    patch_copy(which, 1).wait_recv()

            normalize_queries(group, partial[...] + project(group, 1))

        @pl.when(any_of(task, 0, 2, 6))
        def _():
            pair = pair_of(task)
            for part in (1, 0):
                for route in range(routes + 1):
                    y_copy(part, pair, route).wait_recv()
            value_rows[pair] = kv_all[pair, 1].reshape(KEYS, BLOCK).T

    def score_piece(task, head, piece, held):
        key = kv_all[pair_of(task), 0, piece // 4, piece % 4 * 2 : piece % 4 * 2 + 2].reshape(PIECE, BLOCK)
        scores = lax.dot_general(
            key, query_all[group_of(task), pair_of(task), head], (((1,), (1,)), ((), ())),
            preferred_element_type=jnp.float32,
        )
        held[piece * PIECE : (piece + 1) * PIECE] = scores
        return jnp.max(scores, axis=0, keepdims=True)

    def blend_piece(task, head, piece, held, largest):
        probability = jnp.exp(held[piece * PIECE : (piece + 1) * PIECE] - largest)
        value = value_rows[
            pair_of(task), head * HDIM : (head + 1) * HDIM, piece * PIECE : (piece + 1) * PIECE
        ]
        return jnp.dot(
            value, probability.astype(jnp.bfloat16), preferred_element_type=jnp.float32
        ), jnp.sum(probability, axis=0, keepdims=True)

    def stage(done_task, done_head, held, largest_ref, next_task, next_head, next_held, next_largest_ref):
        largest = largest_ref[...]
        best = blended = total = None
        for piece in range(KEYS // PIECE):
            tops = score_piece(next_task, next_head, piece, next_held)
            product, part = blend_piece(done_task, done_head, piece, held, largest)
            best = tops if piece == 0 else jnp.maximum(best, tops)
            blended = product if piece == 0 else blended + product
            total = part if piece == 0 else total + part
        next_largest_ref[...] = best
        return blended / total

    prepare(0)
    best = None
    for piece in range(KEYS // PIECE):
        tops = score_piece(0, 0, piece, scores_a)
        best = tops if piece == 0 else jnp.maximum(best, tops)
    largest_a[...] = best

    def one_task(task, carry):
        following = jnp.minimum(task + 1, 4 * PAIRS - 1)

        for at_task, part in ((6, 0), (7, 1)):

            @pl.when(task == at_task)
            def _():
                for which in (4, 5):
                    patch_copy(which, part).wait_recv()
                    patch_copy(which + 7, part).start()

        blended_a[...] = stage(task, 0, scores_a, largest_a, task, 1, scores_b, largest_b)

        @pl.when(task < 4 * PAIRS - 1)
        def _():
            prepare(task + 1)

        second = stage(task, 1, scores_b, largest_b, following, 0, scores_a, largest_a)
        mixed = jnp.concatenate([blended_a[...], second], axis=0).astype(jnp.bfloat16).T
        group, pair = group_of(task), pair_of(task)
        lanes = pl.ds(pl.multiple_of(pair * BLOCK, BLOCK), BLOCK)
        attended[group, :, :, :, lanes] = mixed.reshape(2, 2, HALF, BLOCK)
        @pl.when(group == 0)
        def _():
            for k in range(2):
                out_copy(group, pair, 1, k).start()
                out_own(pair, k).start()

        @pl.when(group > 0)
        def _():
            for dc in range(2):
                for k in range(2):
                    out_copy(group, pair, dc, k).start()

        return carry

    lax.fori_loop(0, 4 * PAIRS, one_task, 0)

    for which in range(10):
        weight_copy(which).wait_send()
    for part in range(2):
        for pair in range(PAIRS):
            for route in range(routes):
                kv_copy(part, pair, route).wait_send()
            for route in range(routes + 1):
                y_copy(part, pair, route).wait_send()
    for which in range(13):
        for part in range(2):
            patch_copy(which, part).wait_send()

    def finish(group, carry):
        for pair in range(PAIRS):
            for k in range(2):
                out_copy(group, pair, 1, k).wait()

                @pl.when(group == 0)
                def _():
                    out_own(pair, k).wait()

                @pl.when(group > 0)
                def _():
                    out_copy(group, pair, 0, k).wait()

        return carry

    lax.fori_loop(0, 4, finish, 0)


def per_device(patches, weight_codes, block_scales, key_proj, value_proj, query_gain, key_gain):
    bf16, f32 = jnp.bfloat16, jnp.float32
    dma = pltpu.SemaphoreType.DMA
    anywhere = pl.BlockSpec(memory_space=pl.ANY)
    in_vmem = pl.BlockSpec(memory_space=pltpu.VMEM)
    mixed = pl.pallas_call(
        kernel,
        out_shape=jax.ShapeDtypeStruct((1, TOKENS, FEATURES), bf16),
        in_specs=[
            anywhere, anywhere, pl.BlockSpec(memory_space=pltpu.SMEM), anywhere, anywhere, in_vmem, in_vmem,
        ],
        out_specs=anywhere,
        scratch_shapes=[
            pltpu.VMEM((4, 2, 2, HALF, FEATURES), bf16),
            pltpu.VMEM((8, ROWS, COLS), bf16),
            pltpu.VMEM((2, TOKENS, FEATURES), bf16),
            pltpu.VMEM((PAIRS, 2, 2, 8, TOKENS, BLOCK), bf16),
            pltpu.VMEM((ROWS, COLS), jnp.int32),
            pltpu.VMEM((4, PAIRS, 2, 2 * TOKENS, BLOCK), bf16),
            pltpu.VMEM((4, 2, 2, HALF, COLS), bf16),
            pltpu.VMEM((PAIRS, BLOCK, KEYS), bf16),
            pltpu.VMEM((KEYS, 2 * TOKENS), f32),
            pltpu.VMEM((KEYS, 2 * TOKENS), f32),
            pltpu.VMEM((1, 2 * TOKENS), f32),
            pltpu.VMEM((1, 2 * TOKENS), f32),
            pltpu.VMEM((HDIM, 2 * TOKENS), f32),
            pltpu.VMEM((2 * TOKENS, COLS), f32),
            dma((5,)), dma((10,)), dma((10,)), dma((2, PAIRS, 7)), dma((2, PAIRS, 7)), dma((2, PAIRS, 8)),
            dma((2, PAIRS, 8)), dma((13, 2)), dma((13, 2)), dma((4, PAIRS, 2, 2)), dma((4, PAIRS, 2, 2)),
        ],
        compiler_params=pltpu.CompilerParams(
            collective_id=0, has_side_effects=True, vmem_limit_bytes=60 * 1024 * 1024
        ),
        name="project_attend",
    )(
        patches, weight_codes, block_scales, key_proj, value_proj,
        query_gain.reshape(1, FEATURES), key_gain.reshape(1, FEATURES),
    )
    def place(source, target):
        target[...] = source[...]
    return pl.pallas_call(
        place,
        out_shape=jax.ShapeDtypeStruct((1, TOKENS, FEATURES), bf16),
        grid=(2,),
        in_specs=[pl.BlockSpec((1, TOKENS // 2, FEATURES), lambda i: (0, i, 0))],
        out_specs=pl.BlockSpec((1, TOKENS // 2, FEATURES), lambda i: (0, i, 0)),
        name="place",
    )(mixed)


def solution(mesh):
    grid = Mesh(mesh.devices.reshape(4, 2, 2, 2, 4), AXES)
    seq, fsdp = ("z", "yh", "c"), ("yl", "x")
    placed = (
        P(fsdp, seq, None), P(fsdp, None), P(fsdp, None), P(fsdp, seq, None), P(fsdp, seq, None), P(), P(),
    )
    return jax.shard_map(
        per_device, mesh=grid, in_specs=placed, out_specs=P(fsdp, seq, None), check_vma=False
    )
```
